256 devices in a mesh: groups: 4 (over x, y), seq: 64 (over z, core).
Axes of the slice: x: 2, y: 2, z: 32, core: 2. Of those that a mesh axis runs over, the one named last changes fastest.
The devices are a block of a 4x8x32 slice.
Arguments:
- queries: bfloat16 [65536, 4096], P(('groups', 'seq')), parts along dimension 0, may hold values from -6 to 6
- keys: bfloat16 [65536, 2048], P(('groups', 'seq')), parts along dimension 0, may hold values from -6 to 6
- values: bfloat16 [65536, 2048], P(('groups', 'seq')), parts along dimension 0, may hold values from -6 to 6
- doc_blocks: int32 [32], P('groups'), parts along dimension 0, may hold values from 1 to 32, 128 in all
Outputs:
- attended: bfloat16 [65536, 4096], P(('groups', 'seq')), parts along dimension 0
The draws below stay inside these ranges and needn't reach their ends.
There are 4 independent parts, one for each index of `groups`. The reference program is written for one: setup_inputs(seed, part) draws one part's arguments, and reference() takes and returns one part's arrays. A program takes and returns all parts, laid end to end along the dimension named above; each array names one. Nothing has to cross between parts.
Inputs may be any that keep to these rules, and one draw needn't show every extreme that they name: `doc_blocks`: the lengths add up to 128; the longest document has exactly 32 units.
All inputs are finite; a program needn't handle non-finite values.
Results may differ from the reference program's by a relative error of at most 0.004.
Values may be sent and summed in bfloat16 or wider, within the bound.
A program may use at most 64 MiB of HBM per device.

```python
import math
import jax
import jax.numpy as jnp
import numpy as np
from jax import lax

HEADS = 32
KV_HEADS = 16
DH = 128
BLK = 128
DOCS = 8
TOKENS = 16384


def draw_keys(key, part):
    own_key = jax.random.fold_in(key, 11)
    background = jnp.clip(jax.random.normal(own_key, (TOKENS, KV_HEADS * DH), jnp.float32), -6.0, 6.0)
    return background.astype(jnp.bfloat16)


def draw_queries(key, part):
    own_key = jax.random.fold_in(key, 17)
    background = jnp.clip(jax.random.normal(own_key, (TOKENS, HEADS * DH), jnp.float32), -6.0, 6.0)
    return background.astype(jnp.bfloat16)


def levels(key, dims, pieces, low, high):
    def one(dim, shards_of):
        draws = jax.random.uniform(jax.random.fold_in(jax.random.fold_in(key, 6), dim), (shards_of,), jnp.float32, low / len(pieces), high / len(pieces))
        return jnp.repeat(jnp.exp(draws), dims[dim] // shards_of).reshape((-1,) + (1,) * (len(dims) - dim - 1))

    loudness = one(*pieces[0])
    for cut in pieces[1:]:
        loudness = loudness * one(*cut)
    return loudness


def length_profile(amount, total, most, slope):
    portions = [(1 << 20) // math.isqrt(rank ** slope) + 1 for rank in range(2, amount + 1)]
    spare, counts = total - most - (amount - 1), [1] * (amount - 1)
    while spare > 0:
        movable = [i for i in range(amount - 1) if counts[i] < most]
        mass, budget = sum([portions[i] for i in movable]), spare
        for i in movable:
            extra = min(most - counts[i], max(1, budget * portions[i] // mass), spare)
            counts[i] = counts[i] + extra
            spare = spare - extra
    return np.array([most] + counts)


def ragged_sizes(stream_key, number_of, total, limit, lean):
    if number_of == 2:
        one = jax.random.randint(stream_key, (), max(1, total - limit), min(limit, total - 1) + 1)
        return jnp.stack([one, total - one])
    tallies = jnp.asarray(length_profile(number_of, total, limit, lean), jnp.int32)
    twos = (number_of - 1) // 2
    source_of, sink = tallies[1:1 + 2 * twos:2], tallies[2:2 + 2 * twos:2]
    margin = jnp.minimum(source_of - 1, limit - sink)
    shifted = jax.random.randint(jax.random.fold_in(stream_key, 1), (twos,), 0, 1 << 20) % (margin + 1)
    tallies = tallies.at[1:1 + 2 * twos:2].set(source_of - shifted).at[2:2 + 2 * twos:2].set(sink + shifted)
    return tallies[jax.random.permutation(jax.random.fold_in(stream_key, 2), number_of)]


def bell_draw(key, dims, width, most, pieces=(), held_as=jnp.bfloat16):
    gain = levels(key, dims, pieces, -0.22, 0.18) if pieces else 1.0
    entries = jax.random.normal(key, dims, jnp.float32) * width * gain
    return jnp.minimum(jnp.maximum(entries, -most), most).astype(held_as)


def setup_inputs(seed: int = 0, part: int = 0) -> dict:
    key_list = jax.random.split(jax.random.key(seed), 5)
    own_keys = jax.random.split(jax.random.fold_in(key_list[4], part), 5)
    queries = draw_queries(jax.random.fold_in(jax.random.fold_in(key_list[4], part), 71), part)
    keys = draw_keys(jax.random.fold_in(jax.random.fold_in(key_list[4], part), 71), part)
    values = bell_draw(own_keys[2], (TOKENS, KV_HEADS * DH), 1.0, 6.0, ((0, 64),))
    doc_blocks = ragged_sizes(own_keys[3], DOCS, TOKENS // BLK, TOKENS // BLK // 4, 2).astype(jnp.int32)
    return dict(queries=queries, keys=keys, values=values, doc_blocks=doc_blocks)


score_scale = 144.0 ** -0.5


def reference(queries, keys, values, doc_blocks):
    lengths = doc_blocks.astype(jnp.int32) * BLK
    doc_ends = jnp.cumsum(lengths).astype(jnp.int32)
    doc_starts = (doc_ends - lengths).astype(jnp.int32)
    positions = jnp.arange(TOKENS, dtype=jnp.int32)
    doc_number = jnp.sum((positions[:, None] >= doc_ends[None, :]).astype(jnp.int32), axis=1).astype(jnp.int32)
    own_start = jnp.sum(jnp.where(doc_number[:, None] == jnp.arange(DOCS, dtype=jnp.int32)[None, :], doc_starts[None, :], 0), axis=1).astype(jnp.int32)
    query_heads = queries.reshape(TOKENS, KV_HEADS, HEADS // KV_HEADS, DH)
    key_heads = keys.reshape(TOKENS, KV_HEADS, DH)
    value_heads = values.reshape(TOKENS, KV_HEADS, DH)
    tile_rows = min(256, TOKENS)
    window_rows = min(TOKENS, TOKENS // 4 + tile_rows)

    def one_tile(block_index):
        first_row = (block_index * tile_rows).astype(jnp.int32)
        query_tile = lax.dynamic_slice_in_dim(query_heads, first_row, tile_rows, 0).astype(jnp.float32)
        key_first = jnp.clip(first_row + tile_rows - window_rows, 0, TOKENS - window_rows).astype(jnp.int32)
        key_tile = lax.dynamic_slice_in_dim(key_heads, key_first, window_rows, 0).astype(jnp.float32)
        value_tile = lax.dynamic_slice_in_dim(value_heads, key_first, window_rows, 0).astype(jnp.float32)
        scores = jnp.einsum("qgsd,kgd->gsqk", query_tile, key_tile) * score_scale
        tile_pos = first_row + jnp.arange(tile_rows, dtype=jnp.int32)
        tile_start = lax.dynamic_slice_in_dim(own_start, first_row, tile_rows, 0)
        key_pos = key_first + jnp.arange(window_rows, dtype=jnp.int32)
        visible = (key_pos[None, :] >= tile_start[:, None]) & (key_pos[None, :] <= tile_pos[:, None])
        row_max = jnp.max(jnp.where(visible, scores, -1e30), axis=-1)
        weights = jnp.where(visible, jnp.exp(scores - row_max[..., None]), 0.0)
        row_total = jnp.sum(weights, axis=-1)
        rounded = lax.optimization_barrier(weights.astype(jnp.bfloat16)).astype(jnp.float32)
        blended = jnp.einsum("gsqk,kgd->gsqd", rounded, value_tile) / row_total[..., None]
        return blended.transpose(2, 0, 1, 3).reshape(tile_rows, HEADS * DH).astype(jnp.bfloat16)

    blocks = lax.map(one_tile, jnp.arange(TOKENS // tile_rows, dtype=jnp.int32))
    return blocks.reshape(TOKENS, HEADS * DH)
```

```python
import functools

import jax
import jax.numpy as jnp
from jax import lax
from jax.experimental import pallas as pl
from jax.experimental.pallas import tpu as pltpu
from jax.sharding import PartitionSpec as P

DH = 128
BLK = 128
MAX_UNITS = 32
MESH = pl.DeviceIdType.MESH
LOG2E = 1.4426950408889634
SCALE = 144.0 ** (-0.5) * LOG2E
HIDDEN = -1e30
FLOOR = -1e29


def kernel(
    chips, reach, tail, docs_ref, q_hbm, k_hbm, v_hbm, o_hbm,
    q_all, own, got, run_max, run_sum, acc, result,
    load_sem, pair_send, pair_recv, ring_send, ring_recv, out_sem, back_send, back_recv,
):
    rows = q_hbm.shape[0]
    both = 2 * rows
    keys_here = own.shape[0]
    heads_here = q_all.shape[0]
    ratio = heads_here // keys_here
    blocks = both // BLK
    me = lax.axis_index("seq")
    core = lax.rem(me, 2)
    chip = lax.div(me, 2)
    partner = me + 1 - 2 * core
    right = lax.rem(chip + 1, chips) * 2 + core
    left = lax.rem(chip + chips - 1, chips) * 2 + core

    barrier = pltpu.get_barrier_semaphore()
    for source in (left, partner):
        pl.semaphore_signal(barrier, inc=1, device_id={"seq": source}, device_id_type=MESH)
    pl.semaphore_wait(barrier, 2)

    mine = pl.ds(pl.multiple_of(core * rows, rows), rows)
    theirs = pl.ds(pl.multiple_of((1 - core) * rows, rows), rows)

    def columns(head):
        return pl.ds(pl.multiple_of(head * DH, DH), DH)

    def pieces(index, side, place):
        first = side * keys_here + index
        listed = [
            (k_hbm.at[:, columns(first)], own.at[index, 0, place], index),
            (v_hbm.at[:, columns(first)], own.at[index, 1, place], keys_here + index),
        ]
        for j in range(ratio):
            head = index * ratio + j
            listed.append(
                (
                    q_hbm.at[:, columns(side * heads_here + head)],
                    q_all.at[head, place],
                    2 * keys_here + head,
                )
            )
        return listed

    def local_copy(entry):
        return pltpu.make_async_copy(entry[0], entry[1], load_sem.at[entry[2]])

    def pair_copy(entry):
        return pltpu.make_async_remote_copy(
            src_ref=entry[0], dst_ref=entry[1],
            send_sem=pair_send.at[entry[2]], recv_sem=pair_recv.at[entry[2]],
            device_id={"seq": partner}, device_id_type=MESH,
        )

    def start_kv(g, carry):
        for entry in pieces(g, 1 - core, mine)[:2]:
            pair_copy(entry).start()
        for entry in pieces(g, core, mine)[:2]:
            local_copy(entry).start()
        return carry

    def start_q(g, carry):
        for entry in pieces(g, 1 - core, mine)[2:]:
            pair_copy(entry).start()
        for entry in pieces(g, core, mine)[2:]:
            local_copy(entry).start()
        return carry

    lax.fori_loop(0, keys_here, start_kv, 0)
    lax.fori_loop(0, keys_here, start_q, 0)

    def hop(source, step, g, partial):
        rows_sent = pl.ds(both - tail, tail) if partial else pl.ds(0, both)
        return pltpu.make_async_remote_copy(
            src_ref=source.at[:, rows_sent], dst_ref=got.at[step, g, :, rows_sent],
            send_sem=ring_send.at[step, g], recv_sem=ring_recv.at[step, g],
            device_id={"seq": right}, device_id_type=MESH,
        )

    def first_send(g, carry):
        for entry in pieces(g, core, mine)[:2]:
            local_copy(entry).wait()
        for entry in pieces(g, 1 - core, theirs)[:2]:
            pair_copy(entry).wait_recv()
        hop(own.at[g], 0, g, reach == 1).start()
        return carry

    lax.fori_loop(0, keys_here, first_send, 0)

    def wait_q(g, carry):
        for entry in pieces(g, core, mine)[2:]:
            local_copy(entry).wait()
        for entry in pieces(g, 1 - core, theirs)[2:]:
            pair_copy(entry).wait_recv()
        return carry

    lax.fori_loop(0, keys_here, wait_q, 0)

    starts = []
    for b in range(blocks):
        block = chip * blocks + b
        end = jnp.int32(0)
        start = jnp.int32(0)
        for d in range(docs_ref.shape[0]):
            end = end + docs_ref[d]
            start = jnp.where(block >= end, end, start)
        starts.append(start * BLK)

    def flash(g, source, first_key, skip, causal):
        count = both - skip
        k = source[0, pl.ds(skip, count), :]
        v = source[1, pl.ds(skip, count), :]
        lane = lax.broadcasted_iota(jnp.int32, (ratio * BLK, count), 1) + (first_key + skip)
        for b in range(blocks):
            span = pl.ds(b * BLK, BLK)
            q = q_all[pl.ds(g * ratio, ratio), span, :].reshape(ratio * BLK, DH)
            s = lax.dot_general(q, k, (((1,), (1,)), ((), ())), preferred_element_type=jnp.float32)
            visible = lane >= starts[b]
            if causal:
                row = lax.broadcasted_iota(jnp.int32, (ratio, BLK, count), 1).reshape(ratio * BLK, count)
                visible = visible & (lane <= row + (chip * both + b * BLK))
            s = jnp.where(visible, s * SCALE, HIDDEN)
            top = jnp.max(s, axis=1, keepdims=True)
            if causal:
                new_max = jnp.maximum(jnp.full((ratio * BLK, DH), FLOOR, jnp.float32), top)
            else:
                old_max = run_max[g, b]
                new_max = jnp.maximum(old_max, top)
            p = jnp.exp2(s - new_max[:, :1])
            total = jnp.sum(p, axis=1, keepdims=True)
            fresh = jnp.dot(p.astype(jnp.bfloat16), v, preferred_element_type=jnp.float32)
            if causal:
                run_sum[g, b] = jnp.broadcast_to(total, (ratio * BLK, DH))
                acc[g, b] = fresh
            else:
                shrink = jnp.exp2(old_max - new_max)
                run_sum[g, b] = run_sum[g, b] * shrink + total
                acc[g, b] = acc[g, b] * shrink + fresh
            run_max[g, b] = new_max

    def own_block(g, carry):
        flash(g, own.at[g], chip * both, 0, True)
        return carry

    lax.fori_loop(0, keys_here, own_block, 0)

    def out_copy(head):
        return pltpu.make_async_copy(
            result.at[head, mine], o_hbm.at[:, columns(core * heads_here + head)], out_sem.at[head]
        )

    def back_copy(head, side):
        return pltpu.make_async_remote_copy(
            src_ref=result.at[head, theirs],
            dst_ref=o_hbm.at[:, columns(side * heads_here + head)],
            send_sem=back_send.at[head], recv_sem=back_recv.at[head],
            device_id={"seq": partner}, device_id_type=MESH,
        )

    def finish(g):
        for b in range(blocks):
            value = (acc[g, b] / run_sum[g, b]).astype(jnp.bfloat16).reshape(ratio, BLK, DH)
            result[pl.ds(g * ratio, ratio), pl.ds(b * BLK, BLK), :] = value

    def send_back(g):
        for j in range(ratio):
            back_copy(g * ratio + j, core).start()
            out_copy(g * ratio + j).start()

    def middle(index, carry):
        step = index // keys_here
        g = index % keys_here
        source = got.at[step, g]
        hop(source, step, g, False).wait_recv()

        @pl.when(step < reach - 2)
        def _():
            hop(source, step + 1, g, False).start()

        @pl.when(step == reach - 2)
        def _():
            hop(source, reach - 1, g, True).start()

        flash(g, source, (chip - 1 - step) * both, 0, False)
        return carry

    lax.fori_loop(0, (reach - 1) * keys_here, middle, 0)

    def last(g, carry):
        source = got.at[reach - 1, g]
        hop(source, reach - 1, g, True).wait_recv()
        flash(g, source, (chip - reach) * both, both - tail, False)
        finish(g)

        @pl.when(g > 0)
        def _():
            send_back(g - 1)

        return carry

    lax.fori_loop(0, keys_here, last, 0)
    send_back(keys_here - 1)

    def drain(g, carry):
        for entry in pieces(g, 1 - core, mine):
            pair_copy(entry).wait_send()
        for step in range(reach):
            hop(own.at[g], step, g, step == reach - 1).wait_send()
        for j in range(ratio):
            head = g * ratio + j
            out_copy(head).wait()
            back_copy(head, core).wait_send()
            back_copy(head, 1 - core).wait_recv()
        return carry

    lax.fori_loop(0, keys_here, drain, 0)


def on_device(queries, keys, values, doc_blocks):
    rows = queries.shape[0]
    both = 2 * rows
    chips = lax.axis_size("seq") // 2
    heads_here = queries.shape[1] // DH // 2
    keys_here = keys.shape[1] // DH // 2
    ratio = heads_here // keys_here
    blocks = both // BLK
    back = (MAX_UNITS - 1) * BLK
    reach = -(-back // both)
    tail = back - (reach - 1) * both
    state = (keys_here, blocks, ratio * BLK, DH)
    pieces = 2 * keys_here + heads_here
    anywhere = pl.BlockSpec(memory_space=pl.ANY)
    return pl.pallas_call(
        functools.partial(kernel, chips, reach, tail),
        out_shape=jax.ShapeDtypeStruct(queries.shape, queries.dtype),
        in_specs=[pl.BlockSpec(memory_space=pltpu.SMEM)] + [anywhere] * 3,
        out_specs=anywhere,
        scratch_shapes=[
            pltpu.VMEM((heads_here, both, DH), jnp.bfloat16),
            pltpu.VMEM((keys_here, 2, both, DH), jnp.bfloat16),
            pltpu.VMEM((reach, keys_here, 2, both, DH), jnp.bfloat16),
            pltpu.VMEM(state, jnp.float32),
            pltpu.VMEM(state, jnp.float32),
            pltpu.VMEM(state, jnp.float32),
            pltpu.VMEM((heads_here, both, DH), jnp.bfloat16),
            pltpu.SemaphoreType.DMA((pieces,)),
            pltpu.SemaphoreType.DMA((pieces,)),
            pltpu.SemaphoreType.DMA((pieces,)),
            pltpu.SemaphoreType.DMA((reach, keys_here)),
            pltpu.SemaphoreType.DMA((reach, keys_here)),
            pltpu.SemaphoreType.DMA((heads_here,)),
            pltpu.SemaphoreType.DMA((heads_here,)),
            pltpu.SemaphoreType.DMA((heads_here,)),
        ],
        compiler_params=pltpu.CompilerParams(
            collective_id=0, has_side_effects=True, vmem_limit_bytes=60 * 1024 * 1024
        ),
        name="forward_attention",
    )(doc_blocks, queries, keys, values)


def solution(mesh):
    token = P(("groups", "seq"), None)
    return jax.shard_map(
        on_device, mesh=mesh, in_specs=(token, token, token, P("groups")),
        out_specs=token, check_vma=False,
    )
```

```python
import functools

import jax
import jax.numpy as jnp
from jax import lax
from jax.experimental import pallas as pl
from jax.experimental.pallas import tpu as pltpu
from jax.sharding import PartitionSpec as P

DH = 128
BLK = 128
MAX_UNITS = 32
MESH = pl.DeviceIdType.MESH
LOG2E = 1.4426950408889634
SCALE = 144.0 ** (-0.5) * LOG2E
HIDDEN = -1e30
FLOOR = -1e29
FAR = 1 << 30


def kernel(
    chips, span, docs_ref, q_hbm, k_hbm, v_hbm, o_hbm,
    q_all, own, turned, got, sent, got_stat, sent_stat, q_got,
    run_max, run_sum, acc, part, part_stat, result,
    load_sem, pair_send, pair_recv, ring_send, ring_recv, stat_send, stat_recv,
    q_send, q_recv, out_sem, back_send, back_recv,
):
    rows = q_hbm.shape[0]
    both = 2 * rows
    keys_here = own.shape[0]
    heads_here = q_all.shape[0]
    ratio = heads_here // keys_here
    blocks = both // BLK
    fixed = keys_here // 2
    me = lax.axis_index("seq")
    core = lax.rem(me, 2)
    chip = lax.div(me, 2)
    partner = me + 1 - 2 * core
    right = lax.rem(chip + 1, chips) * 2 + core
    left = lax.rem(chip + chips - 1, chips) * 2 + core

    barrier = pltpu.get_barrier_semaphore()
    for source in (left, right, partner):
        pl.semaphore_signal(barrier, inc=1, device_id={"seq": source}, device_id_type=MESH)
    pl.semaphore_wait(barrier, 3)

    mine = pl.ds(pl.multiple_of(core * rows, rows), rows)
    theirs = pl.ds(pl.multiple_of((1 - core) * rows, rows), rows)

    def columns(head):
        return pl.ds(pl.multiple_of(head * DH, DH), DH)

    def block_rows(b):
        return pl.ds(pl.multiple_of(b * BLK, BLK), BLK)

    def kv_pieces(index, side, place):
        first = side * keys_here + index
        return [
            (k_hbm.at[:, columns(first)], own.at[index, 0, place], index),
            (v_hbm.at[:, columns(first)], own.at[index, 1, place], keys_here + index),
        ]

    def q_pieces(index, side, place):
        listed = []
        for j in range(ratio):
            head = index * ratio + j
            listed.append(
                (
                    q_hbm.at[:, columns(side * heads_here + head)],
                    q_all.at[head, place],
                    2 * keys_here + head,
                )
            )
        return listed

    def local_copy(entry):
        return pltpu.make_async_copy(entry[0], entry[1], load_sem.at[entry[2]])

    def pair_copy(entry):
        return pltpu.make_async_remote_copy(
            src_ref=entry[0], dst_ref=entry[1],
            send_sem=pair_send.at[entry[2]], recv_sem=pair_recv.at[entry[2]],
            device_id={"seq": partner}, device_id_type=MESH,
        )

    def load(kind, index):
        for entry in kind(index, 1 - core, mine):
            pair_copy(entry).start()
        for entry in kind(index, core, mine):
            local_copy(entry).start()

    def arrive(kind, index):
        for entry in kind(index, core, mine):
            local_copy(entry).wait()
        for entry in kind(index, 1 - core, theirs):
            pair_copy(entry).wait_recv()

    def hop(source, phase, slot, b):
        return pltpu.make_async_remote_copy(
            src_ref=source, dst_ref=got.at[phase, slot, b],
            send_sem=ring_send.at[phase % 2, slot, b], recv_sem=ring_recv.at[phase, slot, b],
            device_id={"seq": right}, device_id_type=MESH,
        )

    def stat_hop(phase, slot, b):
        return pltpu.make_async_remote_copy(
            src_ref=sent_stat.at[phase % 2, slot, b], dst_ref=got_stat.at[phase, slot, b],
            send_sem=stat_send.at[phase % 2, slot, b], recv_sem=stat_recv.at[phase, slot, b],
            device_id={"seq": right}, device_id_type=MESH,
        )

    def q_hop(source, phase, slot, b):
        return pltpu.make_async_remote_copy(
            src_ref=source, dst_ref=q_got.at[phase, slot, b],
            send_sem=q_send.at[phase, slot, b], recv_sem=q_recv.at[phase, slot, b],
            device_id={"seq": left}, device_id_type=MESH,
        )

    def own_q(phase, b):
        return q_all.at[pl.ds((fixed + phase) * ratio, ratio), block_rows(b)]

    load(kv_pieces, 0)
    load(q_pieces, fixed)

    def start_rest(g, carry):
        load(kv_pieces, fixed + g)

        @pl.when(g > 0)
        def _():
            load(q_pieces, fixed + g)
            load(kv_pieces, g)

        load(q_pieces, g)
        return carry

    lax.fori_loop(0, fixed, start_rest, 0)

    arrive(kv_pieces, 0)
    for b in range(blocks):
        hop(own.at[0, :, block_rows(b)], 0, 0, b).start()
    arrive(q_pieces, fixed)
    for b in range(blocks):
        q_hop(own_q(0, b), 0, 0, b).start()

    def wait_rest(g, carry):
        arrive(kv_pieces, fixed + g)

        @pl.when(g > 0)
        def _():
            arrive(q_pieces, fixed + g)
            arrive(kv_pieces, g)

        arrive(q_pieces, g)
        turned[g] = own[fixed + g, 1].astype(jnp.float32).T.astype(jnp.bfloat16)
        return carry

    lax.fori_loop(0, fixed, wait_rest, 0)

    def unit(index):
        total = jnp.int32(0)
        start = jnp.int32(0)
        end = jnp.int32(FAR)
        for d in range(docs_ref.shape[0]):
            total = total + docs_ref[d]
            start = jnp.where(index >= total, total, start)
            end = jnp.minimum(end, jnp.where(index >= total, FAR, total))
        return start, end

    first = chip * blocks
    here_start, here_end = unit(first + blocks - 1)
    keys_from = jnp.where(here_end > first + blocks, here_start, FAR)
    _, before_end = unit(first - 1)
    sums_to = jnp.where((before_end > first) & (chip > 0), before_end, 0)

    def flash(g, b, k, v, first_key, causal):
        start = unit(first + b)[0] * BLK
        lane = lax.broadcasted_iota(jnp.int32, (ratio * BLK, both), 1) + first_key
        q = q_all[pl.ds(g * ratio, ratio), block_rows(b), :].reshape(ratio * BLK, DH)
        s = lax.dot_general(q, k, (((1,), (1,)), ((), ())), preferred_element_type=jnp.float32)
        visible = lane >= start
        if causal:
            row = lax.broadcasted_iota(jnp.int32, (ratio, BLK, both), 1).reshape(ratio * BLK, both)
            visible = visible & (lane <= row + (first_key + b * BLK))
        s = jnp.where(visible, s * SCALE, HIDDEN)
        top = jnp.max(s, axis=1, keepdims=True)
        if causal:
            new_max = jnp.maximum(jnp.full((ratio * BLK, DH), FLOOR, jnp.float32), top)
        else:
            old_max = run_max[g, b]
            new_max = jnp.maximum(old_max, top)
        p = jnp.exp2(s - new_max[:, :1])
        total = jnp.sum(p, axis=1, keepdims=True)
        fresh = jnp.dot(p.astype(jnp.bfloat16), v, preferred_element_type=jnp.float32)
        if causal:
            run_sum[g, b] = jnp.broadcast_to(total, (ratio * BLK, DH))
            acc[g, b] = fresh
        else:
            shrink = jnp.exp2(old_max - new_max)
            run_sum[g, b] = run_sum[g, b] * shrink + total
            acc[g, b] = acc[g, b] * shrink + fresh
        run_max[g, b] = new_max

    def partial(g, b, q, place, block, causal):
        start = unit(block)[0] * BLK
        k = own[fixed + g, 0]
        s = lax.dot_general(k, q, (((1,), (1,)), ((), ())), preferred_element_type=jnp.float32)
        key = lax.broadcasted_iota(jnp.int32, (both, ratio * BLK), 0) + first * BLK
        visible = key >= start
        if causal:
            lane = lax.broadcasted_iota(jnp.int32, (both, ratio * BLK), 1)
            visible = visible & (key <= (lane & (BLK - 1)) + block * BLK)
        s = jnp.where(visible, s * SCALE, HIDDEN)
        top = jnp.maximum(jnp.max(s, axis=0, keepdims=True), FLOOR)
        p = jnp.exp2(s - top)
        total = jnp.sum(p, axis=0, keepdims=True)
        summed = jnp.dot(turned[g], p.astype(jnp.bfloat16), preferred_element_type=jnp.float32)
        for j in range(ratio):
            lanes = slice(j * BLK, (j + 1) * BLK)
            part[g % 2, place, b, j] = summed[:, lanes]
            part_stat[g % 2, place, b, pl.ds(j, 1), :] = top[:, lanes]
            part_stat[g % 2, place, b, pl.ds(ratio + j, 1), :] = total[:, lanes]

    def out_copy(head):
        return pltpu.make_async_copy(
            result.at[head, mine], o_hbm.at[:, columns(core * heads_here + head)], out_sem.at[head]
        )

    def back_copy(head, side):
        return pltpu.make_async_remote_copy(
            src_ref=result.at[head, theirs],
            dst_ref=o_hbm.at[:, columns(side * heads_here + head)],
            send_sem=back_send.at[head], recv_sem=back_recv.at[head],
            device_id={"seq": partner}, device_id_type=MESH,
        )

    def finish(g):
        for b in range(blocks):
            value = (acc[g, b] / run_sum[g, b]).astype(jnp.bfloat16).reshape(ratio, BLK, DH)
            result[pl.ds(g * ratio, ratio), pl.ds(b * BLK, BLK), :] = value

    def send_back(g):
        for j in range(ratio):
            back_copy(g * ratio + j, core).start()
            out_copy(g * ratio + j).start()

    def free_slot(phase, slot, b):
        @pl.when(phase >= 2)
        def _():
            hop(sent.at[0, slot, b], phase, slot, b).wait_send()

        @pl.when(phase >= 3)
        def _():
            stat_hop(phase, slot, b).wait_send()

    def chosen(block):
        return jnp.full((BLK, DH), block, jnp.int32) >= keys_from

    def step(index, carry):
        phase = index // (span * blocks)
        slot = (index // blocks) % span
        b = index % blocks
        block_in = first - (1 + slot) * blocks + b

        hop(got.at[phase, slot, b], phase, slot, b).wait_recv()

        @pl.when(phase == 0)
        def _():
            @pl.when(slot < span - 1)
            def _():
                sent[0, slot + 1, b] = got[0, slot, b]

        @pl.when(phase > 0)
        def _():
            stat_hop(phase, slot, b).wait_recv()
            turn = (phase - 1) % 2
            place = jnp.where(slot == span - 1, span, span - 2 - slot)
            usable = jnp.full((1, BLK), block_in + span * blocks, jnp.int32) < sums_to
            sums = []
            for j in range(ratio):
                came = jnp.where(usable, got_stat[phase, slot, b, pl.ds(j, 1), :], HIDDEN)
                top = part_stat[turn, place, b, pl.ds(j, 1), :]
                total = part_stat[turn, place, b, pl.ds(ratio + j, 1), :]
                peak = jnp.maximum(came, top)
                keep = jnp.exp2(came - peak)
                add = jnp.exp2(top - peak)
                weight = jnp.maximum(keep + add * total, 1.0)
                share = 1.0 / weight
                mixed = got[phase, slot, b, j].astype(jnp.float32) * (keep * share) + part[
                    turn, place, b, j
                ] * (add * share)
                sums.append((mixed, peak + jnp.log2(weight)))

            @pl.when(slot < span - 1)
            def _():
                free_slot(phase, slot + 1, b)
                pick = chosen(block_in)
                for j in range(ratio):
                    sent[phase % 2, slot + 1, b, j] = jnp.where(
                        pick, got[phase, slot, b, j], sums[j][0].astype(jnp.bfloat16)
                    )
                    sent_stat[phase % 2, slot + 1, b, pl.ds(j, 1), :] = sums[j][1]

            @pl.when(slot == span - 1)
            def _():
                for j in range(ratio):
                    head = (fixed + phase - 1) * ratio + j
                    result[head, block_rows(b), :] = sums[j][0].T.astype(jnp.bfloat16)

        @pl.when(phase < fixed)
        def _():
            q_hop(q_got.at[phase, slot, b], phase, slot, b).wait_recv()

            @pl.when(slot < span - 1)
            def _():
                q_hop(q_got.at[phase, slot, b], phase, slot + 1, b).start()

        @pl.when(slot < span - 1)
        def _():
            hop(sent.at[phase % 2, slot + 1, b], phase, slot + 1, b).start()

            @pl.when(phase > 0)
            def _():
                stat_hop(phase, slot + 1, b).start()

        @pl.when(phase < fixed)
        def _():
            partial(
                phase, b, q_got[phase, slot, b].reshape(ratio * BLK, DH), slot,
                first + (1 + slot) * blocks + b, False,
            )

            @pl.when(slot == 0)
            def _():
                q = q_all[pl.ds((fixed + phase) * ratio, ratio), block_rows(b), :]
                partial(phase, b, q.reshape(ratio * BLK, DH), span, first + b, True)
                flash(phase, b, own[phase, 0], own[phase, 1], first * BLK, True)

            @pl.when(slot == span - 1)
            def _():
                after = phase + 1
                free_slot(after, 0, b)
                pick = chosen(first + b)
                head = jnp.minimum(after, fixed - 1)
                for j in range(ratio):
                    top = part_stat[phase % 2, span - 1, b, pl.ds(j, 1), :]
                    weight = jnp.maximum(part_stat[phase % 2, span - 1, b, pl.ds(ratio + j, 1), :], 1.0)
                    summed = part[phase % 2, span - 1, b, j] * (1.0 / weight)
                    sent[after % 2, 0, b, j] = jnp.where(
                        pick, own[head, j, block_rows(b), :], summed.astype(jnp.bfloat16)
                    )
                    sent_stat[after % 2, 0, b, pl.ds(j, 1), :] = top + jnp.log2(weight)

                @pl.when(after < fixed)
                def _():
                    q_hop(own_q(after, b), after, 0, b).start()

                hop(sent.at[after % 2, 0, b], after, 0, b).start()
                stat_hop(after, 0, b).start()

        last = index // blocks - 1

        @pl.when((last >= 0) & (last < fixed * span))
        def _():
            g = last // span
            place = last % span
            k = got[g, place, :, 0].reshape(both, DH)
            v = got[g, place, :, 1].reshape(both, DH)
            flash(g, b, k, v, (chip - 1 - place) * both, False)

        @pl.when((phase == fixed) & (slot >= 1) & (slot <= fixed) & (b == 0))
        def _():
            finish(slot - 1)
            send_back(slot - 1)

        @pl.when((phase > 0) & (slot == span - 1) & (b == blocks - 1))
        def _():
            send_back(fixed + phase - 1)

        return carry

    lax.fori_loop(0, (fixed + 1) * span * blocks, step, 0)

    def drain(g, carry):
        for entry in kv_pieces(g, 1 - core, mine) + q_pieces(g, 1 - core, mine):
            pair_copy(entry).wait_send()
        for j in range(ratio):
            head = g * ratio + j
            out_copy(head).wait()
            back_copy(head, core).wait_send()
            back_copy(head, 1 - core).wait_recv()
        return carry

    lax.fori_loop(0, keys_here, drain, 0)

    def drain_ring(index, carry):
        slot = index // blocks
        b = index % blocks
        for phase in range(fixed):
            q_hop(q_got.at[phase, slot, b], phase, slot, b).wait_send()
        for phase in range(max(fixed - 1, 0), fixed + 1):
            hop(sent.at[0, slot, b], phase, slot, b).wait_send()
        for phase in range(max(fixed - 1, 1), fixed + 1):
            stat_hop(phase, slot, b).wait_send()
        return carry

    lax.fori_loop(0, span * blocks, drain_ring, 0)


def on_device(queries, keys, values, doc_blocks):
    rows = queries.shape[0]
    both = 2 * rows
    chips = lax.axis_size("seq") // 2
    heads_here = queries.shape[1] // DH // 2
    keys_here = keys.shape[1] // DH // 2
    ratio = heads_here // keys_here
    fixed = keys_here // 2
    blocks = both // BLK
    span = MAX_UNITS // blocks
    state = (fixed, blocks, ratio * BLK, DH)
    slots = (span, blocks)
    pieces = 2 * keys_here + heads_here
    dma = pltpu.SemaphoreType.DMA
    anywhere = pl.BlockSpec(memory_space=pl.ANY)
    return pl.pallas_call(
        functools.partial(kernel, chips, span),
        out_shape=jax.ShapeDtypeStruct(queries.shape, queries.dtype),
        in_specs=[pl.BlockSpec(memory_space=pltpu.SMEM)] + [anywhere] * 3,
        out_specs=anywhere,
        scratch_shapes=[
            pltpu.VMEM((heads_here, both, DH), jnp.bfloat16),
            pltpu.VMEM((keys_here, 2, both, DH), jnp.bfloat16),
            pltpu.VMEM((fixed, DH, both), jnp.bfloat16),
            pltpu.VMEM((fixed + 1,) + slots + (2, BLK, DH), jnp.bfloat16),
            pltpu.VMEM((2,) + slots + (2, BLK, DH), jnp.bfloat16),
            pltpu.VMEM((fixed + 1,) + slots + (ratio, BLK), jnp.float32),
            pltpu.VMEM((2,) + slots + (ratio, BLK), jnp.float32),
            pltpu.VMEM((fixed,) + slots + (ratio, BLK, DH), jnp.bfloat16),
            pltpu.VMEM(state, jnp.float32),
            pltpu.VMEM(state, jnp.float32),
            pltpu.VMEM(state, jnp.float32),
            pltpu.VMEM((2, span + 1, blocks, ratio, DH, BLK), jnp.float32),
            pltpu.VMEM((2, span + 1, blocks, 2 * ratio, BLK), jnp.float32),
            pltpu.VMEM((heads_here, both, DH), jnp.bfloat16),
            dma((pieces,)),
            dma((pieces,)),
            dma((pieces,)),
            dma((2,) + slots),
            dma((fixed + 1,) + slots),
            dma((2,) + slots),
            dma((fixed + 1,) + slots),
            dma((fixed,) + slots),
            dma((fixed,) + slots),
            dma((heads_here,)),
            dma((heads_here,)),
            dma((heads_here,)),
        ],
        compiler_params=pltpu.CompilerParams(
            collective_id=0, has_side_effects=True, vmem_limit_bytes=62 * 1024 * 1024
        ),
        name="two_way_attention",
    )(doc_blocks, queries, keys, values)


def solution(mesh):
    token = P(("groups", "seq"), None)
    return jax.shard_map(
        on_device, mesh=mesh, in_specs=(token, token, token, P("groups")),
        out_specs=token, check_vma=False,
    )
```

```python
import functools

import jax
import jax.numpy as jnp
from jax import lax
from jax.experimental import pallas as pl
from jax.experimental.pallas import tpu as pltpu
from jax.sharding import PartitionSpec as P

DH = 128
BLK = 128
MAX_UNITS = 32
MESH = pl.DeviceIdType.MESH
LOG2E = 1.4426950408889634
SCALE = 144.0 ** (-0.5) * LOG2E
HIDDEN = -1e30
FLOOR = -1e29
FAR = 1 << 30


def kernel(
    chips, span, docs_ref, q_hbm, k_hbm, v_hbm, o_hbm,
    q_all, own, turned, got, sent, got_stat, sent_stat, q_got,
    run_max, run_sum, acc, part, part_stat, result,
    load_sem, pair_send, pair_recv, ring_send, ring_recv, stat_send, stat_recv,
    q_send, q_recv, out_sem, back_send, back_recv,
):
    rows = q_hbm.shape[0]
    both = 2 * rows
    key_slots = own.shape[0]
    ratio = q_all.shape[0] // key_slots
    blocks = both // BLK
    half = k_hbm.shape[1] // DH // 2
    me = lax.axis_index("seq")
    core = lax.rem(me, 2)
    chip = lax.div(me, 2)
    partner = me + 1 - 2 * core
    right = lax.rem(chip + 1, chips) * 2 + core
    left = lax.rem(chip + chips - 1, chips) * 2 + core
    has_left = chip > 0
    has_right = chip < chips - 1

    moved = half // 2 - 1 + core
    fixed = moved + 1
    keys_here = fixed + moved
    key_base = core * (half - 1)
    moved_there = half // 2 - core
    fixed_there = moved_there + 1
    keys_there = fixed_there + moved_there
    base_there = (1 - core) * (half - 1)

    barrier = pltpu.get_barrier_semaphore()

    def greet(device):
        pl.semaphore_signal(barrier, inc=1, device_id={"seq": device}, device_id_type=MESH)

    greet(partner)
    pl.when(has_left)(lambda: greet(left))
    pl.when(has_right)(lambda: greet(right))
    pl.semaphore_wait(barrier, 1 + jnp.minimum(chip, 1) + jnp.minimum(chips - 1 - chip, 1))

    mine = pl.ds(pl.multiple_of(core * rows, rows), rows)
    theirs = pl.ds(pl.multiple_of((1 - core) * rows, rows), rows)

    def columns(head):
        return pl.ds(pl.multiple_of(head * DH, DH), DH)

    def block_rows(b):
        return pl.ds(pl.multiple_of(b * BLK, BLK), BLK)

    def kv_pieces(index, base, place):
        from_head = columns(base + index)
        return [
            (k_hbm.at[:, from_head], own.at[index, 0, place], index),
            (v_hbm.at[:, from_head], own.at[index, 1, place], key_slots + index),
        ]

    def q_pieces(index, base, place):
        listed = []
        for j in range(ratio):
            head = index * ratio + j
            listed.append(
                (
                    q_hbm.at[:, columns(base * ratio + head)],
                    q_all.at[head, place],
                    2 * key_slots + head,
                )
            )
        return listed

    def local_copy(entry):
        return pltpu.make_async_copy(entry[0], entry[1], load_sem.at[entry[2]])

    def pair_copy(entry):
        return pltpu.make_async_remote_copy(
            src_ref=entry[0], dst_ref=entry[1],
            send_sem=pair_send.at[entry[2]], recv_sem=pair_recv.at[entry[2]],
            device_id={"seq": partner}, device_id_type=MESH,
        )

    def give(kind, index):
        for entry in kind(index, base_there, mine):
            pair_copy(entry).start()

    def take(kind, index):
        for entry in kind(index, key_base, mine):
            local_copy(entry).start()

    def arrive(kind, index):
        for entry in kind(index, key_base, mine):
            local_copy(entry).wait()
        for entry in kind(index, key_base, theirs):
            pair_copy(entry).wait_recv()

    def hop(source, phase, slot, b):
        return pltpu.make_async_remote_copy(
            src_ref=source, dst_ref=got.at[phase, slot, b],
            send_sem=ring_send.at[phase % 2, slot, b], recv_sem=ring_recv.at[phase, slot, b],
            device_id={"seq": right}, device_id_type=MESH,
        )

    def stat_hop(phase, slot, b):
        return pltpu.make_async_remote_copy(
            src_ref=sent_stat.at[phase % 2, slot, b], dst_ref=got_stat.at[phase, slot, b],
            send_sem=stat_send.at[phase % 2, slot, b], recv_sem=stat_recv.at[phase, slot, b],
            device_id={"seq": right}, device_id_type=MESH,
        )

    def q_hop(source, phase, slot, b):
        return pltpu.make_async_remote_copy(
            src_ref=source, dst_ref=q_got.at[phase, slot, b],
            send_sem=q_send.at[phase, slot, b], recv_sem=q_recv.at[phase, slot, b],
            device_id={"seq": left}, device_id_type=MESH,
        )

    def own_q(phase, b):
        return q_all.at[pl.ds((fixed + phase) * ratio, ratio), block_rows(b)]

    give(kv_pieces, 0)
    take(kv_pieces, 0)
    pl.when(moved_there > 0)(lambda: give(q_pieces, fixed_there))
    pl.when(moved > 0)(lambda: take(q_pieces, fixed))

    def give_rest(g, carry):
        pl.when(g > 0)(lambda: give(kv_pieces, g))
        pl.when(g != fixed_there)(lambda: give(q_pieces, g))
        return carry

    def take_rest(g, carry):
        pl.when(g > 0)(lambda: take(kv_pieces, g))
        pl.when(g != fixed)(lambda: take(q_pieces, g))
        return carry

    lax.fori_loop(0, keys_there, give_rest, 0)
    lax.fori_loop(0, keys_here, take_rest, 0)

    arrive(kv_pieces, 0)

    @pl.when(has_right)
    def _():
        for b in range(blocks):
            hop(own.at[0, :, block_rows(b)], 0, 0, b).start()

    @pl.when(moved > 0)
    def _():
        arrive(q_pieces, fixed)

        @pl.when(has_left)
        def _():
            for b in range(blocks):
                q_hop(own_q(0, b), 0, 0, b).start()

    def wait_rest(g, carry):
        pl.when(g > 0)(lambda: arrive(kv_pieces, g))
        pl.when(g != fixed)(lambda: arrive(q_pieces, g))
        return carry

    lax.fori_loop(0, keys_here, wait_rest, 0)

    def turn_values(g, carry):
        turned[g] = own[fixed + g, 1].astype(jnp.float32).T.astype(jnp.bfloat16)
        return carry

    lax.fori_loop(0, moved, turn_values, 0)

    def unit(index):
        total = jnp.int32(0)
        start = jnp.int32(0)
        end = jnp.int32(FAR)
        for d in range(docs_ref.shape[0]):
            total = total + docs_ref[d]
            start = jnp.where(index >= total, total, start)
            end = jnp.minimum(end, jnp.where(index >= total, FAR, total))
        return start, end

    first = chip * blocks
    here_start, here_end = unit(first + blocks - 1)
    keys_from = jnp.where(here_end > first + blocks, here_start, FAR)
    _, before_end = unit(first - 1)
    sums_to = jnp.where((before_end > first) & (chip > 0), before_end, 0)

    def flash(g, b, k, v, first_key, causal):
        start = unit(first + b)[0] * BLK
        lane = lax.broadcasted_iota(jnp.int32, (ratio * BLK, both), 1) + first_key
        q = q_all[pl.ds(g * ratio, ratio), block_rows(b), :].reshape(ratio * BLK, DH)
        s = lax.dot_general(q, k, (((1,), (1,)), ((), ())), preferred_element_type=jnp.float32)
        visible = lane >= start
        if causal:
            row = lax.broadcasted_iota(jnp.int32, (ratio, BLK, both), 1).reshape(ratio * BLK, both)
            visible = visible & (lane <= row + (first_key + b * BLK))
        s = jnp.where(visible, s * SCALE, HIDDEN)
        top = jnp.max(s, axis=1, keepdims=True)
        if causal:
            new_max = jnp.maximum(jnp.full((ratio * BLK, DH), FLOOR, jnp.float32), top)
        else:
            old_max = run_max[g, b]
            new_max = jnp.maximum(old_max, top)
        p = jnp.exp2(s - new_max[:, :1])
        total = jnp.sum(p, axis=1, keepdims=True)
        fresh = jnp.dot(p.astype(jnp.bfloat16), v, preferred_element_type=jnp.float32)
        if causal:
            run_sum[g, b] = jnp.broadcast_to(total, (ratio * BLK, DH))
            acc[g, b] = fresh
        else:
            shrink = jnp.exp2(old_max - new_max)
            run_sum[g, b] = run_sum[g, b] * shrink + total
            acc[g, b] = acc[g, b] * shrink + fresh
        run_max[g, b] = new_max

    def partial(g, b, q, place, block, causal):
        start = unit(block)[0] * BLK
        k = own[fixed + g, 0]
        s = lax.dot_general(k, q, (((1,), (1,)), ((), ())), preferred_element_type=jnp.float32)
        key = lax.broadcasted_iota(jnp.int32, (both, ratio * BLK), 0) + first * BLK
        visible = key >= start
        if causal:
            lane = lax.broadcasted_iota(jnp.int32, (both, ratio * BLK), 1)
            visible = visible & (key <= (lane & (BLK - 1)) + block * BLK)
        s = jnp.where(visible, s * SCALE, HIDDEN)
        top = jnp.maximum(jnp.max(s, axis=0, keepdims=True), FLOOR)
        p = jnp.exp2(s - top)
        total = jnp.sum(p, axis=0, keepdims=True)
        summed = jnp.dot(turned[g], p.astype(jnp.bfloat16), preferred_element_type=jnp.float32)
        for j in range(ratio):
            lanes = slice(j * BLK, (j + 1) * BLK)
            part[g % 2, place, b, j] = summed[:, lanes]
            part_stat[g % 2, place, b, pl.ds(j, 1), :] = top[:, lanes]
            part_stat[g % 2, place, b, pl.ds(ratio + j, 1), :] = total[:, lanes]

    def out_copy(head):
        return pltpu.make_async_copy(
            result.at[head, mine], o_hbm.at[:, columns(key_base * ratio + head)], out_sem.at[head]
        )

    def back_copy(head, base):
        return pltpu.make_async_remote_copy(
            src_ref=result.at[head, theirs],
            dst_ref=o_hbm.at[:, columns(base * ratio + head)],
            send_sem=back_send.at[head], recv_sem=back_recv.at[head],
            device_id={"seq": partner}, device_id_type=MESH,
        )

    def finish(g):
        for b in range(blocks):
            value = (acc[g, b] / run_sum[g, b]).astype(jnp.bfloat16).reshape(ratio, BLK, DH)
            result[pl.ds(g * ratio, ratio), pl.ds(b * BLK, BLK), :] = value

    def send_back(g):
        for j in range(ratio):
            back_copy(g * ratio + j, key_base).start()
            out_copy(g * ratio + j).start()

    def free_slot(phase, slot, b):
        @pl.when(phase >= 2)
        def _():
            hop(sent.at[0, slot, b], phase, slot, b).wait_send()

        @pl.when(phase >= 3)
        def _():
            stat_hop(phase, slot, b).wait_send()

    def chosen(block):
        return jnp.full((BLK, DH), block, jnp.int32) >= keys_from

    def forward_flash(last, b):
        g = last // span
        place = last % span

        @pl.when((last >= 0) & (chip - 1 - place >= 0))
        def _():
            k = got[g, place, :, 0].reshape(both, DH)
            v = got[g, place, :, 1].reshape(both, DH)
            flash(g, b, k, v, (chip - 1 - place) * both, False)

    def step(index, carry):
        phase = index // (span * blocks)
        slot = (index // blocks) % span
        b = index % blocks
        block_in = first - (1 + slot) * blocks + b

        @pl.when(has_left)
        def _():
            hop(got.at[phase, slot, b], phase, slot, b).wait_recv()
            pl.when(phase > 0)(lambda: stat_hop(phase, slot, b).wait_recv())

        @pl.when((phase == 0) & (slot < span - 1))
        def _():
            @pl.when(has_left)
            def _():
                sent[0, slot + 1, b] = got[0, slot, b]

            @pl.when(chip == 0)
            def _():
                sent[0, slot + 1, b] = jnp.zeros((2, BLK, DH), jnp.bfloat16)

        @pl.when(phase > 0)
        def _():
            turn = (phase - 1) % 2
            place = jnp.where(slot == span - 1, span, span - 2 - slot)
            home = block_in + span * blocks
            usable = jnp.full((1, BLK), home, jnp.int32) < sums_to
            usable_block = jnp.full((DH, BLK), home, jnp.int32) < sums_to
            sums = []
            for j in range(ratio):
                came = jnp.where(usable, got_stat[phase, slot, b, pl.ds(j, 1), :], HIDDEN)
                top = part_stat[turn, place, b, pl.ds(j, 1), :]
                total = part_stat[turn, place, b, pl.ds(ratio + j, 1), :]
                peak = jnp.maximum(came, top)
                keep = jnp.exp2(came - peak)
                add = jnp.exp2(top - peak)
                weight = jnp.maximum(keep + add * total, 1.0)
                share = 1.0 / weight
                arrived = jnp.where(usable_block, got[phase, slot, b, j].astype(jnp.float32), 0.0)
                mixed = arrived * (keep * share) + part[turn, place, b, j] * (add * share)
                sums.append((mixed, peak + jnp.log2(weight)))

            @pl.when((slot < span - 1) & has_right)
            def _():
                free_slot(phase, slot + 1, b)
                pick = chosen(block_in)
                for j in range(ratio):
                    sent[phase % 2, slot + 1, b, j] = jnp.where(
                        pick, got[phase, slot, b, j], sums[j][0].astype(jnp.bfloat16)
                    )
                    sent_stat[phase % 2, slot + 1, b, pl.ds(j, 1), :] = sums[j][1]

            @pl.when(slot == span - 1)
            def _():
                for j in range(ratio):
                    head = (fixed + phase - 1) * ratio + j
                    result[head, block_rows(b), :] = sums[j][0].T.astype(jnp.bfloat16)

        @pl.when((phase < moved) & (chip + 1 + slot < chips))
        def _():
            q_hop(q_got.at[phase, slot, b], phase, slot, b).wait_recv()

            @pl.when((slot < span - 1) & has_left)
            def _():
                q_hop(q_got.at[phase, slot, b], phase, slot + 1, b).start()

        @pl.when((slot < span - 1) & has_right)
        def _():
            hop(sent.at[phase % 2, slot + 1, b], phase, slot + 1, b).start()

            @pl.when(phase > 0)
            def _():
                stat_hop(phase, slot + 1, b).start()

        @pl.when(phase < moved)
        def _():
            partial(
                phase, b, q_got[phase, slot, b].reshape(ratio * BLK, DH), slot,
                first + (1 + slot) * blocks + b, False,
            )

            @pl.when(slot == 0)
            def _():
                q = q_all[pl.ds((fixed + phase) * ratio, ratio), block_rows(b), :]
                partial(phase, b, q.reshape(ratio * BLK, DH), span, first + b, True)

            @pl.when((slot == span - 1) & has_right)
            def _():
                after = phase + 1
                free_slot(after, 0, b)
                pick = chosen(first + b)
                for j in range(ratio):
                    top = part_stat[phase % 2, span - 1, b, pl.ds(j, 1), :]
                    weight = jnp.maximum(part_stat[phase % 2, span - 1, b, pl.ds(ratio + j, 1), :], 1.0)
                    summed = part[phase % 2, span - 1, b, j] * (1.0 / weight)
                    sent[after % 2, 0, b, j] = jnp.where(
                        pick, own[after, j, block_rows(b), :], summed.astype(jnp.bfloat16)
                    )
                    sent_stat[after % 2, 0, b, pl.ds(j, 1), :] = top + jnp.log2(weight)

                hop(sent.at[after % 2, 0, b], after, 0, b).start()
                stat_hop(after, 0, b).start()

            @pl.when((slot == span - 1) & has_left & (phase + 1 < moved))
            def _():
                q_hop(own_q(phase + 1, b), phase + 1, 0, b).start()

        forward_flash(index // blocks - 1, b)

        @pl.when(slot == 0)
        def _():
            flash(phase, b, own[phase, 0], own[phase, 1], first * BLK, True)

        pl.when((phase > 0) & (slot == 1) & (b == 0))(lambda: finish(phase - 1))
        pl.when((phase > 0) & (slot == 1) & (b == 1))(lambda: send_back(phase - 1))

        @pl.when((phase > 0) & (slot == span - 1) & (b == blocks - 1))
        def _():
            send_back(fixed + phase - 1)

        return carry

    lax.fori_loop(0, fixed * span * blocks, step, 0)

    def final_flash(b, carry):
        forward_flash(fixed * span - 1, b)
        return carry

    lax.fori_loop(0, blocks, final_flash, 0)
    finish(fixed - 1)
    send_back(fixed - 1)

    def drain_given(g, carry):
        for entry in kv_pieces(g, base_there, mine) + q_pieces(g, base_there, mine):
            pair_copy(entry).wait_send()
        for j in range(ratio):
            back_copy(g * ratio + j, base_there).wait_recv()
        return carry

    lax.fori_loop(0, keys_there, drain_given, 0)

    def drain_ring(index, carry):
        slot = index // blocks
        b = index % blocks

        def q_sent(phase, inner):
            q_hop(q_got.at[phase, slot, b], phase, slot, b).wait_send()
            return inner

        def block_sent(phase, inner):
            hop(sent.at[0, slot, b], phase, slot, b).wait_send()
            return inner

        def stat_sent(phase, inner):
            stat_hop(phase, slot, b).wait_send()
            return inner

        @pl.when(has_left & (chip + slot < chips))
        def _():
            lax.fori_loop(0, moved, q_sent, 0)

        @pl.when(has_right)
        def _():
            lax.fori_loop(jnp.maximum(fixed - 2, 0), fixed, block_sent, 0)
            lax.fori_loop(jnp.maximum(fixed - 2, 1), fixed, stat_sent, 0)

        return carry

    lax.fori_loop(0, span * blocks, drain_ring, 0)

    def drain_out(head, carry):
        out_copy(head).wait()
        back_copy(head, key_base).wait_send()
        return carry

    lax.fori_loop(0, keys_here * ratio, drain_out, 0)


def on_device(queries, keys, values, doc_blocks):
    rows = queries.shape[0]
    both = 2 * rows
    chips = lax.axis_size("seq") // 2
    half = keys.shape[1] // DH // 2
    ratio = queries.shape[1] // keys.shape[1]
    key_slots = half + 1
    head_slots = key_slots * ratio
    moved = half // 2
    fixed = moved + 1
    blocks = both // BLK
    span = MAX_UNITS // blocks
    state = (fixed, blocks, ratio * BLK, DH)
    slots = (span, blocks)
    pieces = 2 * key_slots + head_slots
    dma = pltpu.SemaphoreType.DMA
    anywhere = pl.BlockSpec(memory_space=pl.ANY)
    return pl.pallas_call(
        functools.partial(kernel, chips, span),
        out_shape=jax.ShapeDtypeStruct(queries.shape, queries.dtype),
        in_specs=[pl.BlockSpec(memory_space=pltpu.SMEM)] + [anywhere] * 3,
        out_specs=anywhere,
        scratch_shapes=[
            pltpu.VMEM((head_slots, both, DH), jnp.bfloat16),
            pltpu.VMEM((key_slots, 2, both, DH), jnp.bfloat16),
            pltpu.VMEM((moved, DH, both), jnp.bfloat16),
            pltpu.VMEM((fixed,) + slots + (2, BLK, DH), jnp.bfloat16),
            pltpu.VMEM((2,) + slots + (2, BLK, DH), jnp.bfloat16),
            pltpu.VMEM((fixed,) + slots + (ratio, BLK), jnp.float32),
            pltpu.VMEM((2,) + slots + (ratio, BLK), jnp.float32),
            pltpu.VMEM((moved,) + slots + (ratio, BLK, DH), jnp.bfloat16),
            pltpu.VMEM(state, jnp.float32),
            pltpu.VMEM(state, jnp.float32),
            pltpu.VMEM(state, jnp.float32),
            pltpu.VMEM((2, span + 1, blocks, ratio, DH, BLK), jnp.float32),
            pltpu.VMEM((2, span + 1, blocks, 2 * ratio, BLK), jnp.float32),
            pltpu.VMEM((head_slots, both, DH), jnp.bfloat16),
            dma((pieces,)),
            dma((pieces,)),
            dma((pieces,)),
            dma((2,) + slots),
            dma((fixed,) + slots),
            dma((2,) + slots),
            dma((fixed,) + slots),
            dma((moved,) + slots),
            dma((moved,) + slots),
            dma((head_slots,)),
            dma((head_slots,)),
            dma((head_slots,)),
        ],
        compiler_params=pltpu.CompilerParams(
            collective_id=0, has_side_effects=True, vmem_limit_bytes=62 * 1024 * 1024
        ),
        name="two_way_attention",
    )(doc_blocks, queries, keys, values)


def solution(mesh):
    token = P(("groups", "seq"), None)
    return jax.shard_map(
        on_device, mesh=mesh, in_specs=(token, token, token, P("groups")),
        out_specs=token, check_vma=False,
    )
```

```python
import functools

import jax
import jax.numpy as jnp
from jax import lax
from jax.experimental import pallas as pl
from jax.experimental.pallas import tpu as pltpu
from jax.sharding import PartitionSpec as P

DH = 128
BLK = 128
MAX_UNITS = 32
MESH = pl.DeviceIdType.MESH
LOG2E = 1.4426950408889634
SCALE = 144.0 ** (-0.5) * LOG2E
HIDDEN = -1e30
FLOOR = -1e29
FAR = 1 << 30


def kernel(
    chips, span, docs_ref, q_hbm, k_hbm, v_hbm, o_hbm,
    q_all, own, turned, got, sent, got_stat, sent_stat, q_got,
    run_max, run_sum, acc, part, part_stat, result,
    load_sem, pair_send, pair_recv, ring_send, ring_recv, stat_send, stat_recv,
    q_send, q_recv, out_sem, back_send, back_recv,
):
    rows = q_hbm.shape[0]
    both = 2 * rows
    key_slots = own.shape[0]
    ratio = q_all.shape[0] // key_slots
    blocks = both // BLK
    half = k_hbm.shape[1] // DH // 2
    me = lax.axis_index("seq")
    core = lax.rem(me, 2)
    chip = lax.div(me, 2)
    partner = me + 1 - 2 * core
    right = lax.rem(chip + 1, chips) * 2 + core
    left = lax.rem(chip + chips - 1, chips) * 2 + core
    has_left = chip > 0
    has_right = chip < chips - 1

    moved = half // 2 - 1 + core
    fixed = moved + 1
    keys_here = fixed + moved
    key_base = core * (half - 1)
    moved_there = half // 2 - core
    fixed_there = moved_there + 1
    keys_there = fixed_there + moved_there
    base_there = (1 - core) * (half - 1)

    barrier = pltpu.get_barrier_semaphore()

    def greet(device):
        pl.semaphore_signal(barrier, inc=1, device_id={"seq": device}, device_id_type=MESH)

    greet(partner)
    pl.when(has_left)(lambda: greet(left))
    pl.when(has_right)(lambda: greet(right))
    pl.semaphore_wait(barrier, 1 + jnp.minimum(chip, 1) + jnp.minimum(chips - 1 - chip, 1))

    mine = pl.ds(pl.multiple_of(core * rows, rows), rows)
    theirs = pl.ds(pl.multiple_of((1 - core) * rows, rows), rows)

    def columns(head):
        return pl.ds(pl.multiple_of(head * DH, DH), DH)

    def block_rows(b):
        return pl.ds(pl.multiple_of(b * BLK, BLK), BLK)

    def kv_pieces(index, base, place):
        from_head = columns(base + index)
        return [
            (k_hbm.at[:, from_head], own.at[index, 0, place], index),
            (v_hbm.at[:, from_head], own.at[index, 1, place], key_slots + index),
        ]

    def q_pieces(index, base, place):
        listed = []
        for j in range(ratio):
            head = index * ratio + j
            listed.append(
                (
                    q_hbm.at[:, columns(base * ratio + head)],
                    q_all.at[head, place],
                    2 * key_slots + head,
                )
            )
        return listed

    def local_copy(entry):
        return pltpu.make_async_copy(entry[0], entry[1], load_sem.at[entry[2]])

    def pair_copy(entry):
        return pltpu.make_async_remote_copy(
            src_ref=entry[0], dst_ref=entry[1],
            send_sem=pair_send.at[entry[2]], recv_sem=pair_recv.at[entry[2]],
            device_id={"seq": partner}, device_id_type=MESH,
        )

    def give(kind, index):
        for entry in kind(index, base_there, mine):
            pair_copy(entry).start()

    def take(kind, index):
        for entry in kind(index, key_base, mine):
            local_copy(entry).start()

    def arrive(kind, index):
        for entry in kind(index, key_base, mine):
            local_copy(entry).wait()
        for entry in kind(index, key_base, theirs):
            pair_copy(entry).wait_recv()

    def hop(source, phase, slot, b):
        return pltpu.make_async_remote_copy(
            src_ref=source, dst_ref=got.at[phase, slot, b],
            send_sem=ring_send.at[phase % 2, slot, b], recv_sem=ring_recv.at[phase, slot, b],
            device_id={"seq": right}, device_id_type=MESH,
        )

    def stat_hop(phase, slot, b):
        return pltpu.make_async_remote_copy(
            src_ref=sent_stat.at[phase % 2, slot, b], dst_ref=got_stat.at[phase, slot, b],
            send_sem=stat_send.at[phase % 2, slot, b], recv_sem=stat_recv.at[phase, slot, b],
            device_id={"seq": right}, device_id_type=MESH,
        )

    def q_hop(source, phase, slot, b):
        return pltpu.make_async_remote_copy(
            src_ref=source, dst_ref=q_got.at[phase, slot, b],
            send_sem=q_send.at[phase, slot, b], recv_sem=q_recv.at[phase, slot, b],
            device_id={"seq": left}, device_id_type=MESH,
        )

    def own_q(phase, b):
        return q_all.at[pl.ds((fixed + phase) * ratio, ratio), block_rows(b)]

    give(kv_pieces, 0)
    take(kv_pieces, 0)
    pl.when(moved_there > 0)(lambda: give(q_pieces, fixed_there))
    pl.when(moved > 0)(lambda: take(q_pieces, fixed))

    def give_rest(g, carry):
        pl.when(g > 0)(lambda: give(kv_pieces, g))
        pl.when(g != fixed_there)(lambda: give(q_pieces, g))
        return carry

    def take_rest(g, carry):
        pl.when(g > 0)(lambda: take(kv_pieces, g))
        pl.when(g != fixed)(lambda: take(q_pieces, g))
        return carry

    lax.fori_loop(0, keys_there, give_rest, 0)
    lax.fori_loop(0, keys_here, take_rest, 0)

    arrive(kv_pieces, 0)

    @pl.when(has_right)
    def _():
        for b in range(blocks):
            hop(own.at[0, :, block_rows(b)], 0, 0, b).start()

    @pl.when(moved > 0)
    def _():
        arrive(q_pieces, fixed)

        @pl.when(has_left)
        def _():
            for b in range(blocks):
                q_hop(own_q(0, b), 0, 0, b).start()

    def wait_rest(g, carry):
        pl.when(g > 0)(lambda: arrive(kv_pieces, g))
        pl.when(g != fixed)(lambda: arrive(q_pieces, g))
        return carry

    lax.fori_loop(0, keys_here, wait_rest, 0)

    def turn_values(g, carry):
        turned[g] = own[fixed + g, 1].astype(jnp.float32).T.astype(jnp.bfloat16)
        return carry

    lax.fori_loop(0, moved, turn_values, 0)

    def unit(index):
        total = jnp.int32(0)
        start = jnp.int32(0)
        end = jnp.int32(FAR)
        for d in range(docs_ref.shape[0]):
            total = total + docs_ref[d]
            start = jnp.where(index >= total, total, start)
            end = jnp.minimum(end, jnp.where(index >= total, FAR, total))
        return start, end

    first = chip * blocks
    here_start, here_end = unit(first + blocks - 1)
    keys_from = jnp.where(here_end > first + blocks, here_start, FAR)
    _, before_end = unit(first - 1)
    sums_to = jnp.where((before_end > first) & (chip > 0), before_end, 0)

    def flash(g, b, k, v, first_key, causal):
        start = unit(first + b)[0] * BLK
        lane = lax.broadcasted_iota(jnp.int32, (ratio * BLK, both), 1) + first_key
        q = q_all[pl.ds(g * ratio, ratio), block_rows(b), :].reshape(ratio * BLK, DH)
        s = lax.dot_general(q, k, (((1,), (1,)), ((), ())), preferred_element_type=jnp.float32)
        visible = lane >= start
        if causal:
            row = lax.broadcasted_iota(jnp.int32, (ratio, BLK, both), 1).reshape(ratio * BLK, both)
            visible = visible & (lane <= row + (first_key + b * BLK))
        s = jnp.where(visible, s * SCALE, HIDDEN)
        top = jnp.max(s, axis=1, keepdims=True)
        if causal:
            new_max = jnp.maximum(jnp.full((ratio * BLK, DH), FLOOR, jnp.float32), top)
        else:
            old_max = run_max[g, b]
            new_max = jnp.maximum(old_max, top)
        p = jnp.exp2(s - new_max[:, :1])
        total = jnp.sum(p, axis=1, keepdims=True)
        fresh = jnp.dot(p.astype(jnp.bfloat16), v, preferred_element_type=jnp.float32)
        if causal:
            run_sum[g, b] = jnp.broadcast_to(total, (ratio * BLK, DH))
            acc[g, b] = fresh
        else:
            shrink = jnp.exp2(old_max - new_max)
            run_sum[g, b] = run_sum[g, b] * shrink + total
            acc[g, b] = acc[g, b] * shrink + fresh
        run_max[g, b] = new_max

    def partial(g, b, q, place, block, causal):
        start = unit(block)[0] * BLK
        k = own[fixed + g, 0]
        s = lax.dot_general(k, q, (((1,), (1,)), ((), ())), preferred_element_type=jnp.float32)
        key = lax.broadcasted_iota(jnp.int32, (both, ratio * BLK), 0) + first * BLK
        visible = key >= start
        if causal:
            lane = lax.broadcasted_iota(jnp.int32, (both, ratio * BLK), 1)
            visible = visible & (key <= (lane & (BLK - 1)) + block * BLK)
        s = jnp.where(visible, s * SCALE, HIDDEN)
        top = jnp.maximum(jnp.max(s, axis=0, keepdims=True), FLOOR)
        p = jnp.exp2(s - top)
        total = jnp.sum(p, axis=0, keepdims=True)
        summed = jnp.dot(turned[g], p.astype(jnp.bfloat16), preferred_element_type=jnp.float32)
        for j in range(ratio):
            lanes = slice(j * BLK, (j + 1) * BLK)
            part[g % 2, place, b, j] = summed[:, lanes]
            part_stat[g % 2, place, b, pl.ds(j, 1), :] = top[:, lanes]
            part_stat[g % 2, place, b, pl.ds(ratio + j, 1), :] = total[:, lanes]

    def out_copy(head):
        return pltpu.make_async_copy(
            result.at[head, mine], o_hbm.at[:, columns(key_base * ratio + head)], out_sem.at[head]
        )

    def back_copy(head, base):
        return pltpu.make_async_remote_copy(
            src_ref=result.at[head, theirs],
            dst_ref=o_hbm.at[:, columns(base * ratio + head)],
            send_sem=back_send.at[head], recv_sem=back_recv.at[head],
            device_id={"seq": partner}, device_id_type=MESH,
        )

    def finish(g):
        for b in range(blocks):
            value = (acc[g, b] / run_sum[g, b]).astype(jnp.bfloat16).reshape(ratio, BLK, DH)
            result[pl.ds(g * ratio, ratio), pl.ds(b * BLK, BLK), :] = value

    def send_back(g):
        for j in range(ratio):
            back_copy(g * ratio + j, key_base).start()
            out_copy(g * ratio + j).start()

    def chosen(block):
        return jnp.full((BLK, DH), block, jnp.int32) >= keys_from

    def drain_given(g, carry):
        for entry in kv_pieces(g, base_there, mine) + q_pieces(g, base_there, mine):
            pair_copy(entry).wait_send()
        return carry

    def forward_flash(last, b):
        g = last // span
        place = last % span

        @pl.when((last >= 0) & (chip - 1 - place >= 0))
        def _():
            k = got[g, place, :, 0].reshape(both, DH)
            v = got[g, place, :, 1].reshape(both, DH)
            flash(g, b, k, v, (chip - 1 - place) * both, False)

    def step(index, carry):
        phase = index // (span * blocks)
        slot = (index // blocks) % span
        b = index % blocks
        block_in = first - (1 + slot) * blocks + b

        @pl.when(has_left)
        def _():
            hop(got.at[phase, slot, b], phase, slot, b).wait_recv()
            pl.when(phase > 0)(lambda: stat_hop(phase, slot, b).wait_recv())

        @pl.when((phase == 0) & (slot < span - 1))
        def _():
            @pl.when(has_left)
            def _():
                sent[0, slot + 1, b] = got[0, slot, b]

            @pl.when(chip == 0)
            def _():
                sent[0, slot + 1, b] = jnp.zeros((2, BLK, DH), jnp.bfloat16)

        @pl.when(phase > 0)
        def _():
            turn = (phase - 1) % 2
            place = jnp.where(slot == span - 1, span, span - 2 - slot)
            home = block_in + span * blocks
            usable = jnp.full((1, BLK), home, jnp.int32) < sums_to
            usable_block = jnp.full((DH, BLK), home, jnp.int32) < sums_to
            sums = []
            for j in range(ratio):
                came = jnp.where(usable, got_stat[phase, slot, b, pl.ds(j, 1), :], HIDDEN)
                top = part_stat[turn, place, b, pl.ds(j, 1), :]
                total = part_stat[turn, place, b, pl.ds(ratio + j, 1), :]
                peak = jnp.maximum(came, top)
                keep = jnp.exp2(came - peak)
                add = jnp.exp2(top - peak)
                weight = jnp.maximum(keep + add * total, 1.0)
                share = 1.0 / weight
                arrived = jnp.where(usable_block, got[phase, slot, b, j].astype(jnp.float32), 0.0)
                mixed = arrived * (keep * share) + part[turn, place, b, j] * (add * share)
                sums.append((mixed, peak + jnp.log2(weight)))

            @pl.when((slot < span - 1) & has_right)
            def _():
                pick = chosen(block_in)
                for j in range(ratio):
                    sent[phase % 2, slot + 1, b, j] = jnp.where(
                        pick, got[phase, slot, b, j], sums[j][0].astype(jnp.bfloat16)
                    )
                    sent_stat[phase % 2, slot + 1, b, pl.ds(j, 1), :] = sums[j][1]

            @pl.when(slot == span - 1)
            def _():
                for j in range(ratio):
                    head = (fixed + phase - 1) * ratio + j
                    result[head, block_rows(b), :] = sums[j][0].T.astype(jnp.bfloat16)

        @pl.when((phase < moved) & (chip + 1 + slot < chips))
        def _():
            q_hop(q_got.at[phase, slot, b], phase, slot, b).wait_recv()

            @pl.when((slot < span - 1) & has_left)
            def _():
                q_hop(q_got.at[phase, slot, b], phase, slot + 1, b).start()

        @pl.when((slot < span - 1) & has_right)
        def _():
            hop(sent.at[phase % 2, slot + 1, b], phase, slot + 1, b).start()

            @pl.when(phase > 0)
            def _():
                stat_hop(phase, slot + 1, b).start()

        @pl.when(phase < moved)
        def _():
            partial(
                phase, b, q_got[phase, slot, b].reshape(ratio * BLK, DH), slot,
                first + (1 + slot) * blocks + b, False,
            )

            @pl.when(slot == 2)
            def _():
                q = q_all[pl.ds((fixed + phase) * ratio, ratio), block_rows(b), :]
                partial(phase, b, q.reshape(ratio * BLK, DH), span, first + b, True)

            @pl.when((slot == span - 1) & has_right)
            def _():
                after = phase + 1
                pick = chosen(first + b)
                for j in range(ratio):
                    top = part_stat[phase % 2, span - 1, b, pl.ds(j, 1), :]
                    weight = jnp.maximum(part_stat[phase % 2, span - 1, b, pl.ds(ratio + j, 1), :], 1.0)
                    summed = part[phase % 2, span - 1, b, j] * (1.0 / weight)
                    sent[after % 2, 0, b, j] = jnp.where(
                        pick, own[after, j, block_rows(b), :], summed.astype(jnp.bfloat16)
                    )
                    sent_stat[after % 2, 0, b, pl.ds(j, 1), :] = top + jnp.log2(weight)

                hop(sent.at[after % 2, 0, b], after, 0, b).start()
                stat_hop(after, 0, b).start()

            @pl.when((slot == span - 1) & has_left & (phase + 1 < moved))
            def _():
                q_hop(own_q(phase + 1, b), phase + 1, 0, b).start()

        forward_flash(index // blocks - 1, b)

        @pl.when((index < blocks) | ((slot == 4) & (phase < moved)))
        def _():
            g = jnp.where(slot == 4, phase + 1, 0)
            flash(g, b, own[g, 0], own[g, 1], first * BLK, True)

        pl.when((phase > 0) & (slot == 1) & (b == 0))(lambda: finish(phase - 1))
        pl.when((phase > 0) & (slot == 1) & (b == 1))(lambda: send_back(phase - 1))

        @pl.when((phase > 0) & has_right)
        def _():
            hop(sent.at[0, slot, b], phase - 1, slot, b).wait_send()
            pl.when(phase > 1)(lambda: stat_hop(phase - 1, slot, b).wait_send())

        @pl.when((phase > 0) & has_left & (chip + slot < chips))
        def _():
            q_hop(q_got.at[0, slot, b], phase - 1, slot, b).wait_send()

        @pl.when(index == 3 * blocks)
        def _():
            lax.fori_loop(0, keys_there, drain_given, 0)

        @pl.when((phase > 0) & (slot == span - 1) & (b == blocks - 1))
        def _():
            send_back(fixed + phase - 1)

        return carry

    lax.fori_loop(0, fixed * span * blocks, step, 0)

    def final_flash(b, carry):
        forward_flash(fixed * span - 1, b)
        return carry

    lax.fori_loop(0, blocks, final_flash, 0)
    finish(fixed - 1)
    send_back(fixed - 1)

    def drain_ring(index, carry):
        slot = index // blocks
        b = index % blocks
        hop(sent.at[0, slot, b], fixed - 1, slot, b).wait_send()
        pl.when(fixed > 1)(lambda: stat_hop(fixed - 1, slot, b).wait_send())
        return carry

    @pl.when(has_right)
    def _():
        lax.fori_loop(0, span * blocks, drain_ring, 0)

    def drain_out(head, carry):
        out_copy(head).wait()
        back_copy(head, key_base).wait_send()
        return carry

    lax.fori_loop(0, keys_here * ratio, drain_out, 0)

    def drain_back(head, carry):
        back_copy(head, base_there).wait_recv()
        return carry

    lax.fori_loop(0, keys_there * ratio, drain_back, 0)


def on_device(queries, keys, values, doc_blocks):
    rows = queries.shape[0]
    both = 2 * rows
    chips = lax.axis_size("seq") // 2
    half = keys.shape[1] // DH // 2
    ratio = queries.shape[1] // keys.shape[1]
    key_slots = half + 1
    head_slots = key_slots * ratio
    moved = half // 2
    fixed = moved + 1
    blocks = both // BLK
    span = MAX_UNITS // blocks
    state = (fixed, blocks, ratio * BLK, DH)
    slots = (span, blocks)
    pieces = 2 * key_slots + head_slots
    dma = pltpu.SemaphoreType.DMA
    anywhere = pl.BlockSpec(memory_space=pl.ANY)
    return pl.pallas_call(
        functools.partial(kernel, chips, span),
        out_shape=jax.ShapeDtypeStruct(queries.shape, queries.dtype),
        in_specs=[pl.BlockSpec(memory_space=pltpu.SMEM)] + [anywhere] * 3,
        out_specs=anywhere,
        scratch_shapes=[
            pltpu.VMEM((head_slots, both, DH), jnp.bfloat16),
            pltpu.VMEM((key_slots, 2, both, DH), jnp.bfloat16),
            pltpu.VMEM((moved, DH, both), jnp.bfloat16),
            pltpu.VMEM((fixed,) + slots + (2, BLK, DH), jnp.bfloat16),
            pltpu.VMEM((2,) + slots + (2, BLK, DH), jnp.bfloat16),
            pltpu.VMEM((fixed,) + slots + (ratio, BLK), jnp.float32),
            pltpu.VMEM((2,) + slots + (ratio, BLK), jnp.float32),
            pltpu.VMEM((moved,) + slots + (ratio, BLK, DH), jnp.bfloat16),
            pltpu.VMEM(state, jnp.float32),
            pltpu.VMEM(state, jnp.float32),
            pltpu.VMEM(state, jnp.float32),
            pltpu.VMEM((2, span + 1, blocks, ratio, DH, BLK), jnp.float32),
            pltpu.VMEM((2, span + 1, blocks, 2 * ratio, BLK), jnp.float32),
            pltpu.VMEM((head_slots, both, DH), jnp.bfloat16),
            dma((pieces,)),
            dma((pieces,)),
            dma((pieces,)),
            dma((2,) + slots),
            dma((fixed,) + slots),
            dma((2,) + slots),
            dma((fixed,) + slots),
            dma((moved,) + slots),
            dma((moved,) + slots),
            dma((head_slots,)),
            dma((head_slots,)),
            dma((head_slots,)),
        ],
        compiler_params=pltpu.CompilerParams(
            collective_id=0, has_side_effects=True, vmem_limit_bytes=62 * 1024 * 1024
        ),
        name="two_way_attention",
    )(doc_blocks, queries, keys, values)


def solution(mesh):
    token = P(("groups", "seq"), None)
    return jax.shard_map(
        on_device, mesh=mesh, in_specs=(token, token, token, P("groups")),
        out_specs=token, check_vma=False,
    )
```
